32 devices in a mesh: dp: 16 (over z, y, core), tensor: 2 (over x).
Axes of the slice: x: 2, y: 2, z: 4, core: 2. Of those that a mesh axis runs over, the one named last changes fastest.
Arguments:
- attn_out: bfloat16 [12288, 2048], P('dp', 'tensor'), may hold values from -6 to 6
- out_proj_t: bfloat16 [4096, 2048], P(None, 'tensor'), may hold values from -0.09375 to 0.09375
- grad_out: bfloat16 [12288, 4096], P('dp', 'tensor'), may hold values from -6 to 6
- read_weights: float32 [12288, 16], P('dp'), may hold values from 0 to 0.0026041667
- memory_gate: float32 [256, 16], P('dp'), may hold values from -0.2 to 1
- write_pos: int32 [16, 16], P('dp'), may hold values from 0 to 767, as said below
Outputs:
- grad_attn_out: bfloat16 [12288, 2048], P('dp', 'tensor')
- grad_out_proj_t: float32 [4096, 2048], P('dp', 'tensor')
- grad_memory: float32 [256, 4096], P('dp', 'tensor')
The draws below stay inside these ranges and needn't reach their ends.
Inputs may be any that keep to these rules, and one draw needn't show every extreme that they name: `write_pos`: the 16 positions of one segment are distinct.
All inputs are finite; a program needn't handle non-finite values.
Results may differ from the reference program's by a relative error of at most 0.0034.
Values may be sent and summed in bfloat16 or wider, within the bound.
A program may use at most 64 MiB of HBM per device.

```python
import jax
import jax.numpy as jnp
from jax import lax

D = 4096
MEM = 16
SEG = 768
SEGMENT_COUNT = 16
HD = 2048
TOKENS = 12288


def draw_memory_gate(key, part):
    share = 0.5
    gradual_decay = jax.random.uniform(jax.random.fold_in(key, 1), (1, MEM)) < share
    gradual_decay_rate = jnp.exp(-jax.random.uniform(jax.random.fold_in(key, 2), (SEGMENT_COUNT, MEM), jnp.float32, 0.2, 1.5) / SEGMENT_COUNT)
    quick_decay_rate = jax.random.uniform(jax.random.fold_in(key, 3), (SEGMENT_COUNT, MEM), jnp.float32, 0.05, 0.5)
    sudden_spike = jax.random.uniform(jax.random.fold_in(key, 4), (SEGMENT_COUNT, 1)) < 3.0 / SEGMENT_COUNT
    decay_rates = jnp.where(gradual_decay, gradual_decay_rate, quick_decay_rate) * jnp.where(sudden_spike, 0.6, 1.0)
    eye = jnp.eye(MEM, dtype=jnp.float32)
    spread = jnp.clip(jax.random.normal(jax.random.fold_in(key, 5), (SEGMENT_COUNT, MEM, MEM)) * 0.04, -0.2, 0.2)
    gates = spread * (1.0 - eye) + decay_rates[:, :, None] * eye
    return gates.reshape(SEGMENT_COUNT * MEM, MEM).astype(jnp.float32)


def draw_write_pos(key, part):
    keys = jax.random.split(jax.random.fold_in(key, 7), SEGMENT_COUNT)
    picks = jax.vmap(lambda single: jax.random.permutation(single, SEG)[:MEM])(keys)
    return picks.astype(jnp.int32)


def spiked(drawn, stream_key, source, target, parts, factor):
    def block_of(position):
        return (jnp.arange(drawn.shape[position]) // (drawn.shape[position] // parts)).reshape((-1,) + (1,) * (drawn.ndim - 1 - position))

    one_side = jax.random.permutation(stream_key, parts)[block_of(target)]
    second = (block_of(target) + parts // 2) % parts
    return jnp.where((block_of(source) == one_side) | (block_of(source) == second), factor * drawn, drawn)


def levels(rng, dims, cuts, low, high):
    def one(dim, shards_of):
        steps = jax.random.uniform(jax.random.fold_in(jax.random.fold_in(rng, 6), dim), (shards_of,), jnp.float32, low / len(cuts), high / len(cuts))
        return jnp.repeat(jnp.exp(steps), dims[dim] // shards_of).reshape((-1,) + (1,) * (len(dims) - dim - 1))

    factor_of = one(*cuts[0])
    for cut in cuts[1:]:
        factor_of = factor_of * one(*cut)
    return factor_of


def noise(own_key, extent, scale, reach, pieces=(), kind=jnp.bfloat16):
    drawn = scale * jax.random.normal(own_key, extent, jnp.float32)
    if pieces:
        drawn = drawn * levels(own_key, extent, pieces, -0.22, 0.18)
    return jnp.clip(drawn, -reach, reach).astype(kind)


def heavy_noise(own_key, shape, width, most, pieces, heavy, held_as=jnp.bfloat16):
    array = width * jax.random.normal(own_key, shape, jnp.float32)
    if pieces:
        array = array * levels(own_key, shape, pieces, -0.22, 0.18)
    return jnp.clip(spiked(array, jax.random.fold_in(own_key, 3), *heavy), -most, most).astype(held_as)


def setup_inputs(seed: int = 0) -> dict:
    seeds = jax.random.split(jax.random.key(seed), 7)
    attn_out = noise(seeds[0], (TOKENS, HD), 1.0, 6.0, ((0, 16), (1, 2)))
    out_proj_t = noise(seeds[1], (D, HD), D ** -0.5, 0.09375, ((1, 2),))
    grad_out = heavy_noise(seeds[2], (TOKENS, D), 1.0, 6.0, ((0, 16), (1, 2)), (0, 1, 16, 2.0))
    read_weights = jnp.clip(0.0026041667 * jax.random.uniform(seeds[3], (TOKENS, MEM), jnp.float32) ** levels(seeds[3], (TOKENS, MEM), ((0, 16),), -0.2, 0.2), 0.0, 0.0026041667)
    memory_gate = draw_memory_gate(jax.random.fold_in(seeds[6], 71), 0)
    write_pos = draw_write_pos(jax.random.fold_in(seeds[6], 71), 0)
    return {"attn_out": attn_out, "out_proj_t": out_proj_t, "grad_out": grad_out, "read_weights": read_weights, "memory_gate": memory_gate, "write_pos": write_pos}


def reference(attn_out, out_proj_t, grad_out, read_weights, memory_gate, write_pos):
    high = lax.Precision.HIGHEST
    dy = grad_out.astype(jnp.float32).reshape(SEGMENT_COUNT, SEG, D)
    reads = read_weights.reshape(SEGMENT_COUNT, SEG, MEM)
    gates = memory_gate.reshape(SEGMENT_COUNT, MEM, MEM)
    local = jnp.einsum('stm,std->smd', reads, dy, precision=high)

    def sweep(carry, inputs):
        gate, term = inputs
        fresh = jnp.dot(gate.T, carry, precision=high, preferred_element_type=jnp.float32) + term
        return fresh, (fresh, carry)

    start = jnp.zeros((MEM, D), jnp.float32)
    _, (grad_mem, after) = lax.scan(sweep, start, (gates, local), reverse=True)
    places = jnp.arange(SEG, dtype=jnp.int32)
    onehot = (places[None, :, None] == write_pos[:, None, :]).astype(jnp.float32)
    written = jnp.einsum('stm,smd->std', onehot, after, precision=high)
    grad_z = (dy + written).astype(jnp.bfloat16).reshape(TOKENS, D)
    grad_attn = jnp.dot(grad_z, out_proj_t, preferred_element_type=jnp.float32).astype(jnp.bfloat16)
    grad_weight = lax.dot_general(grad_z, attn_out, (((0,), (0,)), ((), ())), preferred_element_type=jnp.float32)
    return grad_attn, grad_weight, grad_mem.reshape(SEGMENT_COUNT * MEM, D)
```

```python
import functools

import jax
import jax.numpy as jnp
from jax import lax
from jax.experimental import pallas as pl
from jax.experimental.pallas import tpu as pltpu
from jax.sharding import PartitionSpec as P

MESH = pl.DeviceIdType.MESH
F32 = jnp.float32
BF16 = jnp.bfloat16


def split3(a):
    hi = a.astype(BF16)
    rest = a - hi.astype(F32)
    mid = rest.astype(BF16)
    low = (rest - mid.astype(F32)).astype(BF16)
    return jnp.concatenate([hi, mid, low], axis=0)


def tdot(a, b):
    return lax.dot_general(a, b, (((0,), (0,)), ((), ())), preferred_element_type=F32)


def kernel(
    n, attn, w_hbm, g, rwt, gate, wpos, out_attn, out_w, out_mem,
    w, attn_p, gx, za, zb, zp, acc, onehot, local, after, after_x,
    lsend, lrecv, asend, arecv, ysend, yrecv, kept, zsend, zrecv, mine,
    w_sem, x_s, x_r, l_s, l_r, a_s, a_r, ax_s, ax_r, t_s, t_r, p_s, p_r, y_s, y_r, z_s, z_r,
):
    d = lax.axis_index("dp")
    t = lax.axis_index("tensor")
    c = lax.rem(d, 2)
    y = lax.rem(d // 2, 2)
    z = d // 4
    nz = n // 4
    seg, half = g.shape
    hd = attn.shape[1]
    slots = rwt.shape[0]
    bw = 2 * half // n
    lw = half // n
    zh = nz // 2
    nq = 2 * zh
    partner = (d + 1 - 2 * c, t)
    xpeer = (d, 1 - t)
    ypeer = (d + 2 - 4 * y, t)
    tile = 256

    def remote(src, dst, ss, rs, dev):
        return pltpu.make_async_remote_copy(
            src_ref=src, dst_ref=dst, send_sem=ss, recv_sem=rs, device_id=dev, device_id_type=MESH
        )

    def peer(o):
        return lax.rem(d + o, n)

    barrier = pltpu.get_barrier_semaphore()
    for o in range(1, n):
        pl.semaphore_signal(barrier, inc=1, device_id=(peer(o), t), device_id_type=MESH)
    pl.semaphore_signal(barrier, inc=1, device_id=xpeer, device_id_type=MESH)

    wcopy = pltpu.make_async_copy(w_hbm, w, w_sem)
    wcopy.start()
    pl.semaphore_wait(barrier, n)

    def place(q):
        zz = q // 2
        yd = 1 - y if q % 2 == 0 else y
        return zz, yd, 2 * zz + yd

    def cols(q, par):
        return pl.ds(pl.multiple_of((2 * place(q)[2] + par) * bw, bw), bw)

    def pair_cols(q):
        return pl.ds(pl.multiple_of(2 * place(q)[2] * bw, 2 * bw), 2 * bw)

    xcopies = []
    for q in range(nq):
        for k in range(2):
            par = 1 - c if k == 0 else c
            i = 2 * q + k
            xcopies.append(
                remote(g.at[:, cols(q, par)], gx.at[:, cols(q, par)], x_s.at[i], x_r.at[i], xpeer)
            )
    early = 3
    for copy in xcopies[:early]:
        copy.start()
    tcopy = remote(attn, attn_p, t_s, t_r, partner)
    tcopy.start()

    three = split3(rwt[...])

    def local_step(i, _):
        at = pl.ds(pl.multiple_of(i * tile, tile), tile)
        r = jnp.dot(three, g[:, at], preferred_element_type=F32)
        local[:, at] = r[:slots] + r[slots : 2 * slots] + r[2 * slots :]
        return 0

    lax.fori_loop(0, half // tile, local_step, 0)

    def msg(o):
        return local[:, pl.ds(pl.multiple_of(peer(o) * lw, lw), lw)]

    lrecv[0, :slots, :] = msg(0)
    lrecv[0, slots:, :] = gate[...]
    lcopies = []
    for o in range(1, n):
        lsend[o, :slots, :] = msg(o)
        lsend[o, slots:, :] = gate[...]
        lcopies.append(remote(lsend.at[o], lrecv.at[o], l_s.at[o], l_r.at[o], (peer(o), t)))
    for copy in lcopies:
        copy.start()

    place_of = lax.broadcasted_iota(jnp.int32, (seg, 3 * slots), 0)
    onehot[...] = jnp.where(place_of == wpos[...], 1.0, 0.0).astype(BF16)
    for copy in lcopies:
        copy.wait_recv()

    def sweep(i, carry):
        s = n - 1 - i
        slot = lax.rem(d - s + n, n)
        target = lax.rem(s - d + n, n)
        asend[target, :slots, :] = carry
        m = lrecv[slot]
        fresh = m[:slots]
        for k in range(slots):
            fresh = fresh + m[slots:, k : k + 1] * carry[k : k + 1, :]
        asend[target, slots:, :] = fresh
        return fresh

    lax.fori_loop(0, n, sweep, jnp.zeros((slots, lw), F32))
    acopies = []
    for o in range(1, n):
        acopies.append(remote(asend.at[o], arecv.at[o], a_s.at[o], a_r.at[o], (peer(o), t)))
    for copy in acopies:
        copy.start()
    for copy in acopies:
        copy.wait_recv()
    for o in range(n):
        src = lax.rem(d - o + n, n)
        at = pl.ds(pl.multiple_of(src * lw, lw), lw)
        m = asend[0] if o == 0 else arecv[o]
        after[:, at] = m[:slots]
        out_mem[:, at] = m[slots:]
    axcopy = remote(after, after_x, ax_s, ax_r, xpeer)
    axcopy.start()
    for copy in xcopies[early:]:
        copy.start()

    def fix(src, aft, dst, at):
        written = jnp.dot(onehot[...], split3(aft[:, at]), preferred_element_type=F32)
        dst[:, at] = (src[:, at].astype(F32) + written).astype(BF16)

    pcopies = []

    def to_partner(zr, q, i):
        copy = remote(zr.at[:, cols(q, 1 - c)], zp.at[i], p_s.at[i], p_r.at[i], partner)
        copy.start()
        pcopies.append(copy)

    ncopies = []
    ycopies = {}

    def grad_block(zr, q, i, first):
        pcopies[i].wait_recv()
        if first:
            tcopy.wait_recv()
        slot = i // 2

        def step(m, _):
            at = pl.ds(pl.multiple_of(m * tile, tile), tile)
            r = tdot(zr[:, cols(q, c)], attn[:, at]) + tdot(zp[i], attn_p[:, at])
            if q % 2 == 0:
                ysend[slot, :, at] = r.astype(BF16)
            else:
                kept[slot, :, at] = r
            return 0

        lax.fori_loop(0, hd // tile, step, 0)
        if q % 2 == 0:
            copy = remote(ysend.at[slot], yrecv.at[slot], y_s.at[slot], y_r.at[slot], ypeer)
            copy.start()
            ycopies[slot] = copy

    def to_owner(h, q, i):
        slot = i // 2
        zd = zh * h + place(q)[0]
        ycopies[slot].wait_recv()
        own = zd == z

        @pl.when(own)
        def _():
            mine[...] = kept[slot] + yrecv[slot].astype(F32)

        @pl.when(jnp.logical_not(own))
        def _():
            o = lax.rem(zd - z + nz, nz)
            zsend[slot] = (kept[slot] + yrecv[slot].astype(F32)).astype(BF16)
            remote(
                zsend.at[slot], zrecv.at[o], z_s.at[slot], z_r.at[o], (zd * 4 + 2 * y + c, t)
            ).start()

        ncopies.append((own, slot, zd))

    for q in range(nq):
        fix(g, after, za, cols(q, 1 - c))
        to_partner(za, q, q)
        fix(g, after, za, cols(q, c))
    for q in range(nq):
        grad_block(za, q, q, q == 0)
    wcopy.wait()

    def own_step(m, _):
        at = pl.ds(pl.multiple_of(m * tile, tile), tile)
        rows = pl.ds(pl.multiple_of(t * half, half), half)
        acc[:, at] = jnp.dot(za[...], w[rows, at], preferred_element_type=F32)
        return 0

    lax.fori_loop(0, hd // tile, own_step, 0)
    for q in range(1, nq, 2):
        to_owner(t, q, q)

    axcopy.wait_recv()
    for q in range(nq):
        i = nq + q
        xcopies[2 * q].wait_recv()
        fix(gx, after_x, zb, cols(q, 1 - c))
        to_partner(zb, q, i)
        xcopies[2 * q + 1].wait_recv()
        fix(gx, after_x, zb, cols(q, c))
        grad_block(zb, q, i, False)

        def other_step(m, _, q=q):
            at = pl.ds(pl.multiple_of(m * tile, tile), tile)
            rows = pl.ds(
                pl.multiple_of((1 - t) * half + 2 * place(q)[2] * bw, 2 * bw), 2 * bw
            )
            r = acc[:, at] + jnp.dot(zb[:, pair_cols(q)], w[rows, at], preferred_element_type=F32)
            if q == nq - 1:
                out_attn[:, at] = r.astype(BF16)
            else:
                acc[:, at] = r
            return 0

        if q % 2 == 1:
            to_owner(1 - t, q, i)
        lax.fori_loop(0, hd // tile, other_step, 0)

    total = mine[...]
    for o in range(1, nz):
        remote(zrecv.at[o], zrecv.at[o], z_s.at[0], z_r.at[o], ypeer).wait_recv()
        total = total + zrecv[o].astype(F32)
    out_w[...] = total

    for copy in xcopies + [tcopy, axcopy] + lcopies + acopies + pcopies + list(ycopies.values()):
        copy.wait_send()
    for own, slot, zd in ncopies:

        @pl.when(jnp.logical_not(own))
        def _():
            remote(zsend.at[slot], zrecv.at[0], z_s.at[slot], z_r.at[0], ypeer).wait_send()


def fused(n, attn_out, out_proj_t, grad_out, read_weights, memory_gate, write_pos):
    seg, half = grad_out.shape
    hd = attn_out.shape[1]
    slots = write_pos.shape[1]
    depth = out_proj_t.shape[0]
    bw, lw, nz = depth // n, half // n, n // 4
    nq = nz
    rwt = read_weights.T
    gate = jnp.pad(memory_gate.T, ((0, 0), (0, lw - slots)))
    wpos = jnp.tile(write_pos, (1, 3))
    V = pltpu.VMEM
    D = pltpu.SemaphoreType.DMA
    vmem = pl.BlockSpec(memory_space=pltpu.VMEM)
    return pl.pallas_call(
        functools.partial(kernel, n),
        out_shape=(
            jax.ShapeDtypeStruct((seg, hd), BF16),
            jax.ShapeDtypeStruct((bw, hd), F32),
            jax.ShapeDtypeStruct((slots, half), F32),
        ),
        in_specs=[vmem, pl.BlockSpec(memory_space=pl.ANY), vmem, vmem, vmem, vmem],
        out_specs=(vmem, vmem, vmem),
        scratch_shapes=[
            V((depth, hd), BF16),
            V((seg, hd), BF16),
            V((seg, half), BF16),
            V((seg, half), BF16),
            V((seg, half), BF16),
            V((2 * nq, seg, bw), BF16),
            V((seg, hd), F32),
            V((seg, 3 * slots), BF16),
            V((slots, half), F32),
            V((slots, half), F32),
            V((slots, half), F32),
            V((n, 2 * slots, lw), F32),
            V((n, 2 * slots, lw), F32),
            V((n, 2 * slots, lw), F32),
            V((n, 2 * slots, lw), F32),
            V((nq, bw, hd), BF16),
            V((nq, bw, hd), BF16),
            V((nq, bw, hd), F32),
            V((nq, bw, hd), BF16),
            V((nz, bw, hd), BF16),
            V((bw, hd), F32),
            D,
            D((2 * nq,)),
            D((2 * nq,)),
            D((n,)),
            D((n,)),
            D((n,)),
            D((n,)),
            D,
            D,
            D,
            D,
            D((2 * nq,)),
            D((2 * nq,)),
            D((nq,)),
            D((nq,)),
            D((nq,)),
            D((nz,)),
        ],
        compiler_params=pltpu.CompilerParams(
            collective_id=0, has_side_effects=True, vmem_limit_bytes=62 * 1024 * 1024
        ),
    )(attn_out, out_proj_t, grad_out, rwt, gate, wpos)


def plain(attn_out, out_proj_t, grad_out, read_weights, memory_gate, write_pos):
    high = lax.Precision.HIGHEST
    seg_len = attn_out.shape[0]
    slots = write_pos.shape[1]
    gate_at_step = memory_gate.T
    dy_cols = grad_out.astype(jnp.float32)
    local = jnp.dot(read_weights.T, dy_cols, precision=high, preferred_element_type=jnp.float32)
    all_gates, all_terms = (
        lax.all_gather(gate_at_step, "dp", axis=0, tiled=True),
        lax.all_gather(local, "dp", axis=0, tiled=True),
    )
    count = lax.axis_size("dp")
    mine = lax.axis_index("dp")

    def sweep(step, carry):
        which = (count - 1 - step).astype(jnp.int32)
        gate = lax.dynamic_slice_in_dim(all_gates, which * slots, slots, 0)
        term = lax.dynamic_slice_in_dim(all_terms, which * slots, slots, 0)
        fresh = jnp.dot(gate, carry, precision=high, preferred_element_type=jnp.float32) + term
        return jnp.where(which > mine, fresh, carry)

    after = lax.fori_loop(0, count, sweep, jnp.zeros_like(local))
    grad_memory = (
        jnp.dot(gate_at_step, after, precision=high, preferred_element_type=jnp.float32) + local
    )
    places = jnp.arange(seg_len, dtype=jnp.int32)
    onehot = (places[:, None] == write_pos[0][None, :]).astype(jnp.float32)
    written = jnp.dot(onehot, after, precision=high, preferred_element_type=jnp.float32)
    grad_z = (dy_cols + written).astype(jnp.bfloat16)
    full_z = lax.all_gather(grad_z, "tensor", axis=1, tiled=True)
    grad_attn = jnp.dot(full_z, out_proj_t, preferred_element_type=jnp.float32).astype(jnp.bfloat16)
    term = lax.dot_general(
        full_z, attn_out, (((0,), (0,)), ((), ())), preferred_element_type=jnp.float32
    )
    grad_weight = lax.psum_scatter(term, "dp", scatter_dimension=0, tiled=True)
    return (grad_attn, grad_weight, grad_memory)


def solution(mesh):
    n = mesh.shape["dp"]
    parts = mesh.shape["tensor"]

    def body(attn_out, out_proj_t, grad_out, read_weights, memory_gate, write_pos):
        half, hd = grad_out.shape[1], attn_out.shape[1]
        fits = (
            parts == 2
            and n % 8 == 0
            and half % (n * 128) == 0
            and half % 256 == 0
            and hd % 256 == 0
            and out_proj_t.shape[0] <= 4096
        )
        args = (attn_out, out_proj_t, grad_out, read_weights, memory_gate, write_pos)
        return fused(n, *args) if fits else plain(*args)

    return jax.shard_map(
        body,
        mesh=mesh,
        in_specs=(
            P("dp", "tensor"),
            P(None, "tensor"),
            P("dp", "tensor"),
            P("dp", None),
            P("dp", None),
            P("dp", None),
        ),
        out_specs=(P("dp", "tensor"), P("dp", "tensor"), P("dp", "tensor")),
        check_vma=False,
    )
```

```python
import functools

import jax
import jax.numpy as jnp
from jax import lax
from jax.experimental import pallas as pl
from jax.experimental.pallas import tpu as pltpu
from jax.sharding import PartitionSpec as P

MESH = pl.DeviceIdType.MESH
F32 = jnp.float32
BF16 = jnp.bfloat16


def split3(a):
    hi = a.astype(BF16)
    rest = a - hi.astype(F32)
    mid = rest.astype(BF16)
    low = (rest - mid.astype(F32)).astype(BF16)
    return jnp.concatenate([hi, mid, low], axis=0)


def tdot(a, b):
    return lax.dot_general(a, b, (((0,), (0,)), ((), ())), preferred_element_type=F32)


def kernel(
    n, attn_hbm, w_hbm, g_hbm, rw, gate, wpos, out_attn, out_w, out_mem,
    g, attn, w, attn_p, gx, za, zb, zp, acc, onehot, local, after, after_x,
    lsend, lrecv, asend, arecv, ysend, yrecv, kept, zsend, zrecv, mine, gpad,
    g_sem, attn_sem, w_sem, x_s, x_r, l_s, l_r, a_s, a_r, ax_s, ax_r, t_s, t_r, p_s, p_r, y_s, y_r, z_s, z_r,
):
    d = lax.axis_index("dp")
    t = lax.axis_index("tensor")
    c = lax.rem(d, 2)
    y = lax.rem(d // 2, 2)
    z = d // 4
    nz = n // 4
    seg, half = g.shape
    hd = attn.shape[1]
    slots = rw.shape[1]
    bw = 2 * half // n
    lw = half // n
    zh = nz // 2
    sub = 128
    ns = bw // sub
    nu = 2 * zh * ns
    partner = (d + 1 - 2 * c, t)
    xpeer = (d, 1 - t)
    ypeer = (d + 2 - 4 * y, t)
    tile = 256

    def remote(src, dst, ss, rs, dev):
        return pltpu.make_async_remote_copy(
            src_ref=src, dst_ref=dst, send_sem=ss, recv_sem=rs, device_id=dev, device_id_type=MESH
        )

    def peer(o):
        return lax.rem(d + o, n)

    barrier = pltpu.get_barrier_semaphore()
    for o in range(1, n):
        pl.semaphore_signal(barrier, inc=1, device_id=(peer(o), t), device_id_type=MESH)
    pl.semaphore_signal(barrier, inc=1, device_id=xpeer, device_id_type=MESH)

    gcopy = pltpu.make_async_copy(g_hbm, g, g_sem)
    gcopy.start()
    attncopy = pltpu.make_async_copy(attn_hbm, attn, attn_sem)
    attncopy.start()
    pl.semaphore_wait(barrier, n)

    def place(h, u):
        r = u // (2 * ns)
        zz = r + h * (zh - 1 - 2 * r)
        yd = 1 - y if (u // ns) % 2 == 0 else y
        return zz, 2 * zz + yd, u % ns

    def cols(h, u, par):
        _, j, piece = place(h, u)
        return pl.ds(pl.multiple_of((2 * j + par) * bw + piece * sub, sub), sub)

    xcopies = []
    for u in range(nu):
        for k in range(2):
            at = cols(t, u, 1 - c if k == 0 else c)
            i = 2 * u + k
            xcopies.append(remote(g_hbm.at[:, at], gx.at[:, at], x_s.at[i], x_r.at[i], xpeer))
    early = 5
    for copy in xcopies[:early]:
        copy.start()
    wcopy = pltpu.make_async_copy(w_hbm, w, w_sem)
    wcopy.start()
    tcopy = remote(attn_hbm, attn_p, t_s, t_r, partner)
    tcopy.start()

    three = split3(rw[...].T)
    gpad[...] = jnp.zeros_like(gpad)
    gpad[:, :slots] = gate[...].T
    gcopy.wait()
    attncopy.wait()

    def local_step(i, _):
        at = pl.ds(pl.multiple_of(i * tile, tile), tile)
        r = jnp.dot(three, g[:, at], preferred_element_type=F32)
        local[:, at] = r[:slots] + r[slots : 2 * slots] + r[2 * slots :]
        return 0

    lax.fori_loop(0, half // tile, local_step, 0)

    def msg(o):
        return local[:, pl.ds(pl.multiple_of(peer(o) * lw, lw), lw)]

    lrecv[0, :slots, :] = msg(0)
    lrecv[0, slots:, :] = gpad[...]
    lcopies = []
    for o in range(1, n):
        lsend[o, :slots, :] = msg(o)
        lsend[o, slots:, :] = gpad[...]
        lcopies.append(remote(lsend.at[o], lrecv.at[o], l_s.at[o], l_r.at[o], (peer(o), t)))
    for copy in lcopies:
        copy.start()

    place_of = lax.broadcasted_iota(jnp.int32, (seg, 3 * slots), 0)
    wide = jnp.concatenate([wpos[...]] * 3, axis=1)
    onehot[...] = jnp.where(place_of == wide, 1.0, 0.0).astype(BF16)
    for copy in lcopies:
        copy.wait_recv()

    def sweep(i, carry):
        s = n - 1 - i
        slot = lax.rem(d - s + n, n)
        target = lax.rem(s - d + n, n)
        asend[target, :slots, :] = carry
        m = lrecv[slot]
        fresh = m[:slots]
        for k in range(slots):
            fresh = fresh + m[slots:, k : k + 1] * carry[k : k + 1, :]
        asend[target, slots:, :] = fresh
        return fresh

    lax.fori_loop(0, n, sweep, jnp.zeros((slots, lw), F32))
    acopies = []
    for o in range(1, n):
        acopies.append(remote(asend.at[o], arecv.at[o], a_s.at[o], a_r.at[o], (peer(o), t)))
    for copy in acopies:
        copy.start()
    for copy in acopies:
        copy.wait_recv()
    for o in range(n):
        src = lax.rem(d - o + n, n)
        at = pl.ds(pl.multiple_of(src * lw, lw), lw)
        m = asend[0] if o == 0 else arecv[o]
        after[:, at] = m[:slots]
        out_mem[:, at] = m[slots:]
    axcopy = remote(after, after_x, ax_s, ax_r, xpeer)
    axcopy.start()
    for copy in xcopies[early:]:
        copy.start()

    def fix(src, aft, dst, at):
        written = jnp.dot(onehot[...], split3(aft[:, at]), preferred_element_type=F32)
        dst[:, at] = (src[:, at].astype(F32) + written).astype(BF16)

    pcopies = []

    def to_partner(zr, h, u, i):
        copy = remote(zr.at[:, cols(h, u, 1 - c)], zp.at[i], p_s.at[i], p_r.at[i], partner)
        copy.start()
        pcopies.append(copy)

    ncopies = []
    ycopies = {}

    def is_other(u):
        return (u // ns) % 2 == 0

    def slot_of(u, i):
        return (i // nu) * (nu // 2) + (u // (2 * ns)) * ns + u % ns

    def grad_block(zr, h, u, i, first):
        pcopies[i].wait_recv()
        if first:
            tcopy.wait_recv()
        slot = slot_of(u, i)

        def step(m, _):
            at = pl.ds(pl.multiple_of(m * tile, tile), tile)
            r = tdot(zr[:, cols(h, u, c)], attn[:, at]) + tdot(zp[i], attn_p[:, at])
            if is_other(u):
                ysend[slot, :, at] = r.astype(BF16)
            else:
                kept[slot, :, at] = r
            return 0

        lax.fori_loop(0, hd // tile, step, 0)
        if is_other(u):
            copy = remote(ysend.at[slot], yrecv.at[slot], y_s.at[slot], y_r.at[slot], ypeer)
            copy.start()
            ycopies[slot] = copy

    def to_owner(h, u, i):
        slot = slot_of(u, i)
        piece = u % ns
        zd = zh * h + place(h, u)[0]
        ycopies[slot].wait_recv()
        own = zd == z

        @pl.when(own)
        def _():
            mine[piece] = kept[slot] + yrecv[slot].astype(F32)

        @pl.when(jnp.logical_not(own))
        def _():
            o = lax.rem(zd - z + nz, nz)
            zsend[slot] = (kept[slot] + yrecv[slot].astype(F32)).astype(BF16)
            remote(
                zsend.at[slot],
                zrecv.at[o, piece],
                z_s.at[slot],
                z_r.at[o, piece],
                (zd * 4 + 2 * y + c, t),
            ).start()

        ncopies.append((own, slot))

    for u in range(nu):
        fix(g, after, za, cols(t, u, 1 - c))
        to_partner(za, t, u, u)
        fix(g, after, za, cols(t, u, c))
    for u in range(nu):
        grad_block(za, t, u, u, u == 0)
    wcopy.wait()
    for u in range(2 * ns):
        if not is_other(u):
            to_owner(t, u, u)

    def own_step(m, _):
        at = pl.ds(pl.multiple_of(m * tile, tile), tile)
        rows = pl.ds(pl.multiple_of(t * half, half), half)
        acc[:, at] = jnp.dot(za[...], w[rows, at], preferred_element_type=F32)
        return 0

    lax.fori_loop(0, hd // tile, own_step, 0)
    for u in range(2 * ns, nu):
        if not is_other(u):
            to_owner(t, u, u)

    oh = 1 - t
    axcopy.wait_recv()
    for u in range(nu):
        i = nu + u
        xcopies[2 * u].wait_recv()
        fix(gx, after_x, zb, cols(oh, u, 1 - c))
        to_partner(zb, oh, u, i)
        xcopies[2 * u + 1].wait_recv()
        fix(gx, after_x, zb, cols(oh, u, c))
        grad_block(zb, oh, u, i, False)
        if not is_other(u):
            to_owner(oh, u, i)

        if (u + 1) % ns == 0:
            wide_at = pl.multiple_of(2 * place(oh, u)[1] * bw, 2 * bw)

            def other_step(m, _, wide_at=wide_at, last=u == nu - 1):
                at = pl.ds(pl.multiple_of(m * tile, tile), tile)
                rows = pl.ds(pl.multiple_of(oh * half + wide_at, 2 * bw), 2 * bw)
                r = acc[:, at] + jnp.dot(
                    zb[:, pl.ds(wide_at, 2 * bw)], w[rows, at], preferred_element_type=F32
                )
                if last:
                    out_attn[:, at] = r.astype(BF16)
                else:
                    acc[:, at] = r
                return 0

            lax.fori_loop(0, hd // tile, other_step, 0)

    for piece in range(ns):
        total = mine[piece]
        for o in range(1, nz):
            remote(
                zrecv.at[o, piece], zrecv.at[o, piece], z_s.at[0], z_r.at[o, piece], ypeer
            ).wait_recv()
            total = total + zrecv[o, piece].astype(F32)
        out_w[pl.ds(piece * sub, sub), :] = total

    for copy in xcopies + [tcopy, axcopy] + lcopies + acopies + pcopies + list(ycopies.values()):
        copy.wait_send()
    for own, slot in ncopies:

        @pl.when(jnp.logical_not(own))
        def _():
            remote(
                zsend.at[slot], zrecv.at[0, 0], z_s.at[slot], z_r.at[0, 0], ypeer
            ).wait_send()


def fused(n, attn_out, out_proj_t, grad_out, read_weights, memory_gate, write_pos):
    seg, half = grad_out.shape
    hd = attn_out.shape[1]
    slots = write_pos.shape[1]
    depth = out_proj_t.shape[0]
    bw, lw, nz = depth // n, half // n, n // 4
    sub = 128
    ns = bw // sub
    nu = nz * ns
    V = pltpu.VMEM
    D = pltpu.SemaphoreType.DMA
    vmem = pl.BlockSpec(memory_space=pltpu.VMEM)
    return pl.pallas_call(
        functools.partial(kernel, n),
        out_shape=(
            jax.ShapeDtypeStruct((seg, hd), BF16),
            jax.ShapeDtypeStruct((bw, hd), F32),
            jax.ShapeDtypeStruct((slots, half), F32),
        ),
        in_specs=[pl.BlockSpec(memory_space=pl.ANY)] * 3 + [vmem] * 3,
        out_specs=(vmem, vmem, vmem),
        scratch_shapes=[
            V((seg, half), BF16),
            V((seg, hd), BF16),
            V((depth, hd), BF16),
            V((seg, hd), BF16),
            V((seg, half), BF16),
            V((seg, half), BF16),
            V((seg, half), BF16),
            V((2 * nu, seg, sub), BF16),
            V((seg, hd), F32),
            V((seg, 3 * slots), BF16),
            V((slots, half), F32),
            V((slots, half), F32),
            V((slots, half), F32),
            V((n, 2 * slots, lw), F32),
            V((n, 2 * slots, lw), F32),
            V((n, 2 * slots, lw), F32),
            V((n, 2 * slots, lw), F32),
            V((nu, sub, hd), BF16),
            V((nu, sub, hd), BF16),
            V((nu, sub, hd), F32),
            V((nu, sub, hd), BF16),
            V((nz, ns, sub, hd), BF16),
            V((ns, sub, hd), F32),
            V((slots, lw), F32),
            D,
            D,
            D,
            D((2 * nu,)),
            D((2 * nu,)),
            D((n,)),
            D((n,)),
            D((n,)),
            D((n,)),
            D,
            D,
            D,
            D,
            D((2 * nu,)),
            D((2 * nu,)),
            D((nu,)),
            D((nu,)),
            D((nu,)),
            D((nz, ns)),
        ],
        compiler_params=pltpu.CompilerParams(
            collective_id=0, has_side_effects=True, vmem_limit_bytes=62 * 1024 * 1024
        ),
    )(attn_out, out_proj_t, grad_out, read_weights, memory_gate, write_pos)


def plain(attn_out, out_proj_t, grad_out, read_weights, memory_gate, write_pos):
    high = lax.Precision.HIGHEST
    seg_len = attn_out.shape[0]
    slots = write_pos.shape[1]
    gate_at_step = memory_gate.T
    dy_cols = grad_out.astype(jnp.float32)
    local = jnp.dot(read_weights.T, dy_cols, precision=high, preferred_element_type=jnp.float32)
    all_gates, all_terms = (
        lax.all_gather(gate_at_step, "dp", axis=0, tiled=True),
        lax.all_gather(local, "dp", axis=0, tiled=True),
    )
    count = lax.axis_size("dp")
    mine = lax.axis_index("dp")

    def sweep(step, carry):
        which = (count - 1 - step).astype(jnp.int32)
        gate = lax.dynamic_slice_in_dim(all_gates, which * slots, slots, 0)
        term = lax.dynamic_slice_in_dim(all_terms, which * slots, slots, 0)
        fresh = jnp.dot(gate, carry, precision=high, preferred_element_type=jnp.float32) + term
        return jnp.where(which > mine, fresh, carry)

    after = lax.fori_loop(0, count, sweep, jnp.zeros_like(local))
    grad_memory = (
        jnp.dot(gate_at_step, after, precision=high, preferred_element_type=jnp.float32) + local
    )
    places = jnp.arange(seg_len, dtype=jnp.int32)
    onehot = (places[:, None] == write_pos[0][None, :]).astype(jnp.float32)
    written = jnp.dot(onehot, after, precision=high, preferred_element_type=jnp.float32)
    grad_z = (dy_cols + written).astype(jnp.bfloat16)
    full_z = lax.all_gather(grad_z, "tensor", axis=1, tiled=True)
    grad_attn = jnp.dot(full_z, out_proj_t, preferred_element_type=jnp.float32).astype(jnp.bfloat16)
    term = lax.dot_general(
        full_z, attn_out, (((0,), (0,)), ((), ())), preferred_element_type=jnp.float32
    )
    grad_weight = lax.psum_scatter(term, "dp", scatter_dimension=0, tiled=True)
    return (grad_attn, grad_weight, grad_memory)


def solution(mesh):
    n = mesh.shape["dp"]
    parts = mesh.shape["tensor"]

    def body(attn_out, out_proj_t, grad_out, read_weights, memory_gate, write_pos):
        half, hd = grad_out.shape[1], attn_out.shape[1]
        fits = (
            parts == 2
            and n % 8 == 0
            and half % (n * 128) == 0
            and half % 256 == 0
            and hd % 256 == 0
            and out_proj_t.shape[0] <= 4096
        )
        args = (attn_out, out_proj_t, grad_out, read_weights, memory_gate, write_pos)
        return fused(n, *args) if fits else plain(*args)

    return jax.shard_map(
        body,
        mesh=mesh,
        in_specs=(
            P("dp", "tensor"),
            P(None, "tensor"),
            P("dp", "tensor"),
            P("dp", None),
            P("dp", None),
            P("dp", None),
        ),
        out_specs=(P("dp", "tensor"), P("dp", "tensor"), P("dp", "tensor")),
        check_vma=False,
    )
```
